16 devices in a mesh: rep: 2 (over y, z), dp: 8 (over x, core).
Axes of the slice: x: 4, y: 2, z: 1, core: 2. Of those that a mesh axis runs over, the one named last changes fastest.
The devices are a block of a 4x4x8 slice.
Arguments:
- a: bfloat16 [16, 4, 4096, 896], P(('rep', 'dp')), parts along dimension 0
- g: bfloat16 [16, 4, 4096, 2560], P(('rep', 'dp')), parts along dimension 0
Outputs:
- output: bfloat16 [8, 896, 2560], P('rep'), parts along dimension 0
There are 2 independent parts. The reference program is written for one: setup_inputs(seed, part) draws one part's arguments, and reference() takes and returns one part's arrays. A program takes and returns all parts, laid end to end along the dimension named above; each array names one.
All inputs are finite; a program needn't handle non-finite values.
Results may differ from the reference program's by a relative error of at most 0.012.
Values are sent between devices in bfloat16 or wider.
A program may use at most 768 MiB of HBM per device.

```python
import jax
import jax.numpy as jnp
from jax import lax

DEVICES = 8
MATRICES = 4
TOKENS = 4096
D = 896
FF = 2560


def setup_inputs(seed: int = 0, part: int = 0) -> dict:
    ka, kg, ks = (jax.random.fold_in(k, part) for k in jax.random.split(jax.random.key(seed), 3))
    size = 2.0 ** jax.random.uniform(ks, (DEVICES, MATRICES, 1, 1), jnp.float32, -1.0, 1.0)
    a = jax.random.normal(ka, (DEVICES, MATRICES, TOKENS, D), jnp.float32)
    g = size * jax.random.normal(kg, (DEVICES, MATRICES, TOKENS, FF), jnp.float32) * (DEVICES * TOKENS) ** -0.5
    return {"a": a.astype(jnp.bfloat16), "g": g.astype(jnp.bfloat16)}


def reference(a, g):
    def take(so_far, one):
        return so_far + jnp.einsum("ntd,ntf->ndf", *one, preferred_element_type=jnp.float32), None

    return lax.scan(take, jnp.zeros((MATRICES, D, FF), jnp.float32), (a, g))[0].astype(jnp.bfloat16)
```

```python
import functools

import jax
import jax.numpy as jnp
from jax import lax
from jax.experimental import pallas as pl
from jax.experimental.pallas import tpu as pltpu
from jax.sharding import PartitionSpec as P

MESH = pl.DeviceIdType.MESH
CORES = 2
COLS = 256
BLOCKS = 2
SLOTS = 10
ACCS = 4
G_SLOTS = 3
LAG_A, LAG_B, LAG_C = 1, 2, 3
LAG_E, LAG_F, LAG_G = 3, 6, 8


def when(cond):
    return pl.when(cond)


def kernel(chips, mats, chunks_per, cols, blocks, a_hbm, g_hbm, out, a_buf, g_buf, acc, sib_out, sib_in, far_out, far_in,
           dir_out, dir_in, sum_out, sum_in, a_sem, g_sem, rs_send, rs_recv, ag_send, ag_recv, pair_send, pair_recv):
    me = lax.axis_index("dp")
    x, c = me // CORES, me % CORES
    chunks = mats * chunks_per
    tokens = a_hbm.shape[1]
    step = tokens // blocks
    partner = {"dp": x * CORES + (1 - c)}

    def chip(delta):
        return lax.rem(x + delta + chips, chips)

    def at(d):
        return {"dp": d * CORES + c}

    def ways(k):
        s = 1 - 2 * lax.rem(k, 2)
        return chip(s), chip(-s)

    far = chip(2)

    def a_copy(n, b):
        rows = pl.ds(b * step, step)
        return pltpu.make_async_copy(a_hbm.at[n, rows], a_buf.at[lax.rem(n, 2), rows], a_sem.at[lax.rem(n, 2), b])

    def g_copy(k, b):
        rows = pl.ds(b * step, step)
        slot = lax.rem(k, G_SLOTS)
        columns = pl.ds(pl.multiple_of(lax.rem(k, chunks_per) * cols, cols), cols)
        return pltpu.make_async_copy(g_hbm.at[k // chunks_per, rows, columns], g_buf.at[slot, rows], g_sem.at[slot, b])

    def remote(src, dst, send, recv, to):
        return pltpu.make_async_remote_copy(src_ref=src, dst_ref=dst, send_sem=send, recv_sem=recv, device_id=to,
                                            device_id_type=MESH)

    def rs(k, kind, src, dst, to):
        slot = lax.rem(k, SLOTS)
        return remote(src.at[slot], dst.at[slot], rs_send.at[kind, slot], rs_recv.at[kind, slot], to)

    def swap(k):
        return rs(k, 0, sib_out, sib_in, partner)

    def hop_far(k):
        return rs(k, 1, far_out, far_in, at(ways(k)[1]))

    def hop_direct(k):
        return rs(k, 2, dir_out, dir_in, at(ways(k)[0]))

    def hop_sum(k):
        return rs(k, 3, sum_out, sum_in, at(ways(k)[1]))

    def place(k, d):
        columns = pl.ds(pl.multiple_of(lax.rem(k, chunks_per) * cols, cols), cols)
        return out.at[k // chunks_per, d, c, :, columns]

    def gather(k, kind, d, to):
        return remote(place(k, d), place(k, d), ag_send.at[kind, k], ag_recv.at[kind, k], at(to))

    def pair(k):
        columns = pl.ds(pl.multiple_of(lax.rem(k, chunks_per) * cols, cols), cols)
        block = out.at[k // chunks_per, :, c, :, columns]
        return remote(block, block, pair_send.at[k], pair_recv.at[k], partner)

    for b in range(blocks):
        a_copy(0, b).start()
        g_copy(0, b).start()
    for b in range(blocks):
        g_copy(1, b).start()
    barrier = pltpu.get_barrier_semaphore()
    for to in (partner, at(chip(1)), at(chip(-1))):
        pl.semaphore_signal(barrier, inc=1, device_id=to, device_id_type=MESH)
    pl.semaphore_wait(barrier, 3)

    def stage_matmul(k):
        @when(k + 2 < chunks)
        def _():
            for b in range(blocks):
                g_copy(k + 2, b).start()

        n, first = k // chunks_per, lax.rem(k, chunks_per) == 0

        @when(first & (n + 1 < mats))
        def _():
            for b in range(blocks):
                a_copy(n + 1, b).start()

        slot, g_slot, a_slot = lax.rem(k, ACCS), lax.rem(k, G_SLOTS), lax.rem(n, 2)
        for b in range(blocks):
            @when(first)
            def _():
                a_copy(n, b).wait()

            g_copy(k, b).wait()
            rows = pl.ds(b * step, step)
            part = lax.dot_general(a_buf[a_slot, rows], g_buf[g_slot, rows], (((0,), (0,)), ((), ())),
                                   preferred_element_type=jnp.float32)
            part = part.reshape(acc.shape[1:])
            if b == 0:
                acc[slot] = part
            else:
                acc[slot] += part

        @when(k >= SLOTS)
        def _():
            swap(k - SLOTS).wait_send()

        rs_slot = lax.rem(k, SLOTS)
        for d in range(chips):
            sib_out[rs_slot, d] = acc[slot, d * CORES + 1 - c].astype(jnp.bfloat16)
        swap(k).start()

    def mine(k, d):
        return acc[lax.rem(k, ACCS), d * CORES + c] + sib_in[lax.rem(k, SLOTS), d].astype(jnp.float32)

    def stage_a(k):
        slot = lax.rem(k, SLOTS)
        swap(k).wait_recv()

        @when(k >= SLOTS)
        def _():
            hop_far(k - SLOTS).wait_send()
            hop_direct(k - SLOTS).wait_send()

        far_out[slot] = mine(k, far).astype(jnp.bfloat16)
        hop_far(k).start()
        dir_out[slot] = mine(k, ways(k)[0]).astype(jnp.bfloat16)
        hop_direct(k).start()

    def stage_b(k):
        slot = lax.rem(k, SLOTS)
        hop_far(k).wait_recv()

        @when(k >= SLOTS)
        def _():
            hop_sum(k - SLOTS).wait_send()

        sum_out[slot] = (mine(k, ways(k)[1]) + far_in[slot].astype(jnp.float32)).astype(jnp.bfloat16)
        hop_sum(k).start()

    def stage_c(k):
        slot = lax.rem(k, SLOTS)
        hop_direct(k).wait_recv()
        hop_sum(k).wait_recv()
        total = mine(k, x) + dir_in[slot].astype(jnp.float32) + sum_in[slot].astype(jnp.float32)
        place(k, x)[...] = total.astype(jnp.bfloat16)

    def stage_d(k):
        forth, back = ways(k)
        gather(k, 0, x, forth).start()
        gather(k, 1, x, back).start()

    def stage_e(k):
        forth, back = ways(k)
        gather(k, 0, back, forth).wait_recv()
        gather(k, 2, back, forth).start()
        gather(k, 1, forth, back).wait_recv()

    def stage_f(k):
        forth, back = ways(k)
        gather(k, 2, far, forth).wait_recv()
        pair(k).start()

    def stage_g(k):
        forth, back = ways(k)
        gather(k, 0, x, forth).wait_send()
        gather(k, 1, x, back).wait_send()
        gather(k, 2, back, forth).wait_send()
        pair(k).wait_recv()
        pair(k).wait_send()

    def spread(t):
        return (t // 3) * 2 + lax.rem(t, 3), lax.rem(t, 3) < 2

    def tick(t, _):
        for stage, lag in ((stage_a, LAG_A), (stage_b, LAG_B), (stage_c, LAG_C)):
            k = t - lag

            @when((k >= 0) & (k < chunks))
            def _():
                stage(k)

        for stage, lag in ((stage_d, 0), (stage_e, LAG_E), (stage_f, LAG_F), (stage_g, LAG_G)):
            u = t - lag - LAG_C
            k, there = spread(jnp.maximum(u, 0))

            @when((u >= 0) & there & (k < chunks))
            def _():
                stage(k)

        @when(t < chunks)
        def _():
            stage_matmul(t)

        return 0

    last = ((chunks - 1) // 2) * 3 + (chunks - 1) % 2
    lax.fori_loop(0, LAG_C + last + LAG_G + 1, tick, 0)

    def drain(i, _):
        k = chunks - SLOTS + i
        swap(k).wait_send()
        hop_far(k).wait_send()
        hop_direct(k).wait_send()
        hop_sum(k).wait_send()
        return 0

    lax.fori_loop(0, SLOTS, drain, 0)


def solution(mesh):
    group = mesh.shape["dp"]
    chips = group // CORES

    def local(a, g):
        _, mats, tokens, rows = a.shape
        width = g.shape[-1]
        piece = rows // group
        chunks_per = width // COLS
        chunks = mats * chunks_per
        shape = (mats, chips, CORES, piece, width)
        bf16, f32 = jnp.bfloat16, jnp.float32
        many, one = (SLOTS, chips, piece, COLS), (SLOTS, piece, COLS)
        dma = pltpu.SemaphoreType.DMA
        flops = 2 * mats * tokens * rows * width
        sums = pl.pallas_call(
            functools.partial(kernel, chips, mats, chunks_per, COLS, BLOCKS),
            out_shape=pltpu.VMEM(shape, bf16),
            in_specs=[pl.BlockSpec(memory_space=pl.ANY)] * 2,
            out_specs=pl.BlockSpec(memory_space=pltpu.VMEM),
            scratch_shapes=[
                pltpu.VMEM((2, tokens, rows), bf16),
                pltpu.VMEM((G_SLOTS, tokens, COLS), bf16),
                pltpu.VMEM((ACCS, group, piece, COLS), f32),
                pltpu.VMEM(many, bf16), pltpu.VMEM(many, bf16),
                pltpu.VMEM(one, bf16), pltpu.VMEM(one, bf16),
                pltpu.VMEM(one, bf16), pltpu.VMEM(one, bf16),
                pltpu.VMEM(one, bf16), pltpu.VMEM(one, bf16),
                dma((2, BLOCKS)), dma((G_SLOTS, BLOCKS)),
                dma((4, SLOTS)), dma((4, SLOTS)),
                dma((3, chunks)), dma((3, chunks)),
                dma((chunks,)), dma((chunks,)),
            ],
            compiler_params=pltpu.CompilerParams(collective_id=0, has_side_effects=True, vmem_limit_bytes=VMEM_LIMIT),
            cost_estimate=pl.CostEstimate(flops=flops, bytes_accessed=a.nbytes + g.nbytes, transcendentals=0),
            name="grad_sums",
        )(a.reshape(a.shape[1:]), g.reshape(g.shape[1:]))
        return sums.reshape(mats, rows, width)

    return jax.shard_map(local, mesh=mesh, in_specs=(P(("rep", "dp")),) * 2, out_specs=P("rep"), check_vma=False)


VMEM_LIMIT = 44 * 2**20
```

```python
import functools

import jax
import jax.numpy as jnp
from jax import lax
from jax.experimental import pallas as pl
from jax.experimental.pallas import tpu as pltpu
from jax.sharding import PartitionSpec as P

MESH = pl.DeviceIdType.MESH
CORES = 2
COLS = 256
BLOCKS = 1
SLOTS = 12
ACCS = 7
G_SLOTS = 3
LAG_A, LAG_B, LAG_C = 2, 4, 6
LAG_E, LAG_F, LAG_G = 5, 10, 13


def when(cond):
    return pl.when(cond)


def kernel(chips, mats, chunks_per, cols, blocks, a_hbm, g_hbm, out, a_buf, g_buf, acc, sib_out, sib_in, far_out, far_in,
           dir_out, dir_in, sum_out, sum_in, a_sem, g_sem, rs_send, rs_recv, ag_send, ag_recv, pair_send, pair_recv):
    me = lax.axis_index("dp")
    x, c = me // CORES, me % CORES
    chunks = mats * chunks_per
    tokens = a_hbm.shape[1]
    step = tokens // blocks
    partner = {"dp": x * CORES + (1 - c)}

    def chip(delta):
        return lax.rem(x + delta + chips, chips)

    def at(d):
        return {"dp": d * CORES + c}

    def ways(k):
        s = 1 - 2 * lax.rem(k, 2)
        return chip(s), chip(-s)

    far = chip(2)

    def a_copy(n, b):
        rows = pl.ds(b * step, step)
        return pltpu.make_async_copy(a_hbm.at[n, rows], a_buf.at[lax.rem(n, 2), rows], a_sem.at[lax.rem(n, 2), b])

    def g_copy(k, b):
        rows = pl.ds(b * step, step)
        slot = lax.rem(k, G_SLOTS)
        columns = pl.ds(pl.multiple_of(lax.rem(k, chunks_per) * cols, cols), cols)
        return pltpu.make_async_copy(g_hbm.at[k // chunks_per, rows, columns], g_buf.at[slot, rows], g_sem.at[slot, b])

    def remote(src, dst, send, recv, to):
        return pltpu.make_async_remote_copy(src_ref=src, dst_ref=dst, send_sem=send, recv_sem=recv, device_id=to,
                                            device_id_type=MESH)

    def rs(k, kind, src, dst, to):
        slot = lax.rem(k, SLOTS)
        return remote(src.at[slot], dst.at[slot], rs_send.at[kind, slot], rs_recv.at[kind, slot], to)

    def swap(k):
        return rs(k, 0, sib_out, sib_in, partner)

    def hop_far(k):
        return rs(k, 1, far_out, far_in, at(ways(k)[1]))

    def hop_direct(k):
        return rs(k, 2, dir_out, dir_in, at(ways(k)[0]))

    def hop_sum(k):
        return rs(k, 3, sum_out, sum_in, at(ways(k)[1]))

    def place(k, d):
        columns = pl.ds(pl.multiple_of(lax.rem(k, chunks_per) * cols, cols), cols)
        return out.at[k // chunks_per, d, c, :, columns]

    def gather(k, kind, d, to):
        return remote(place(k, d), place(k, d), ag_send.at[kind, k], ag_recv.at[kind, k], at(to))

    def pair(k):
        columns = pl.ds(pl.multiple_of(lax.rem(k, chunks_per) * cols, cols), cols)
        block = out.at[k // chunks_per, :, c, :, columns]
        return remote(block, block, pair_send.at[k], pair_recv.at[k], partner)

    for b in range(blocks):
        a_copy(0, b).start()
        g_copy(0, b).start()
    for b in range(blocks):
        g_copy(1, b).start()
    barrier = pltpu.get_barrier_semaphore()
    for to in (partner, at(chip(1)), at(chip(-1))):
        pl.semaphore_signal(barrier, inc=1, device_id=to, device_id_type=MESH)
    pl.semaphore_wait(barrier, 3)

    def stage_matmul(k):
        @when(k + 2 < chunks)
        def _():
            for b in range(blocks):
                g_copy(k + 2, b).start()

        n, first = k // chunks_per, lax.rem(k, chunks_per) == 0

        @when(first & (n + 1 < mats))
        def _():
            for b in range(blocks):
                a_copy(n + 1, b).start()

        slot, g_slot, a_slot = lax.rem(k, ACCS), lax.rem(k, G_SLOTS), lax.rem(n, 2)
        for b in range(blocks):
            @when(first)
            def _():
                a_copy(n, b).wait()

            g_copy(k, b).wait()
            rows = pl.ds(b * step, step)
            part = lax.dot_general(a_buf[a_slot, rows], g_buf[g_slot, rows], (((0,), (0,)), ((), ())),
                                   preferred_element_type=jnp.float32)
            part = part.reshape(acc.shape[1:])
            if b == 0:
                acc[slot] = part
            else:
                acc[slot] += part

        @when(k >= SLOTS)
        def _():
            swap(k - SLOTS).wait_send()

        rs_slot = lax.rem(k, SLOTS)
        for d in range(chips):
            sib_out[rs_slot, d] = acc[slot, d * CORES + 1 - c].astype(jnp.bfloat16)
        swap(k).start()

    def mine(k, d):
        return acc[lax.rem(k, ACCS), d * CORES + c] + sib_in[lax.rem(k, SLOTS), d].astype(jnp.float32)

    def stage_a(k):
        slot = lax.rem(k, SLOTS)
        swap(k).wait_recv()

        @when(k >= SLOTS)
        def _():
            hop_far(k - SLOTS).wait_send()
            hop_direct(k - SLOTS).wait_send()

        far_out[slot] = mine(k, far).astype(jnp.bfloat16)
        hop_far(k).start()
        dir_out[slot] = mine(k, ways(k)[0]).astype(jnp.bfloat16)
        hop_direct(k).start()

    def stage_b(k):
        slot = lax.rem(k, SLOTS)
        hop_far(k).wait_recv()

        @when(k >= SLOTS)
        def _():
            hop_sum(k - SLOTS).wait_send()

        sum_out[slot] = (mine(k, ways(k)[1]) + far_in[slot].astype(jnp.float32)).astype(jnp.bfloat16)
        hop_sum(k).start()

    def stage_c(k):
        slot = lax.rem(k, SLOTS)
        hop_direct(k).wait_recv()
        hop_sum(k).wait_recv()
        total = mine(k, x) + dir_in[slot].astype(jnp.float32) + sum_in[slot].astype(jnp.float32)
        place(k, x)[...] = total.astype(jnp.bfloat16)

    def stage_d(k):
        forth, back = ways(k)
        gather(k, 0, x, forth).start()
        gather(k, 1, x, back).start()

    def stage_e(k):
        forth, back = ways(k)
        gather(k, 0, back, forth).wait_recv()
        gather(k, 2, back, forth).start()
        gather(k, 1, forth, back).wait_recv()

    def stage_f(k):
        forth, back = ways(k)
        gather(k, 2, far, forth).wait_recv()
        pair(k).start()

    def stage_g(k):
        forth, back = ways(k)
        gather(k, 0, x, forth).wait_send()
        gather(k, 1, x, back).wait_send()
        gather(k, 2, back, forth).wait_send()
        pair(k).wait_recv()
        pair(k).wait_send()

    def spread(t):
        return (t // 3) * 2 + lax.rem(t, 3), lax.rem(t, 3) < 2

    def tick(t, _):
        for stage, lag in ((stage_a, LAG_A), (stage_b, LAG_B), (stage_c, LAG_C)):
            k = t - lag

            @when((k >= 0) & (k < chunks))
            def _():
                stage(k)

        for stage, lag in ((stage_d, 0), (stage_e, LAG_E), (stage_f, LAG_F), (stage_g, LAG_G)):
            u = t - lag - LAG_C
            k, there = spread(jnp.maximum(u, 0))

            @when((u >= 0) & there & (k < chunks))
            def _():
                stage(k)

        @when(t < chunks)
        def _():
            stage_matmul(t)

        return 0

    last = ((chunks - 1) // 2) * 3 + (chunks - 1) % 2
    lax.fori_loop(0, LAG_C + last + LAG_G + 1, tick, 0)

    def drain(i, _):
        k = chunks - SLOTS + i
        swap(k).wait_send()
        hop_far(k).wait_send()
        hop_direct(k).wait_send()
        hop_sum(k).wait_send()
        return 0

    lax.fori_loop(0, SLOTS, drain, 0)


def solution(mesh):
    group = mesh.shape["dp"]
    chips = group // CORES

    def local(a, g):
        _, mats, tokens, rows = a.shape
        width = g.shape[-1]
        piece = rows // group
        chunks_per = width // COLS
        chunks = mats * chunks_per
        shape = (mats, chips, CORES, piece, width)
        bf16, f32 = jnp.bfloat16, jnp.float32
        many, one = (SLOTS, chips, piece, COLS), (SLOTS, piece, COLS)
        dma = pltpu.SemaphoreType.DMA
        flops = 2 * mats * tokens * rows * width
        sums = pl.pallas_call(
            functools.partial(kernel, chips, mats, chunks_per, COLS, BLOCKS),
            out_shape=pltpu.VMEM(shape, bf16),
            in_specs=[pl.BlockSpec(memory_space=pl.ANY)] * 2,
            out_specs=pl.BlockSpec(memory_space=pltpu.VMEM),
            scratch_shapes=[
                pltpu.VMEM((2, tokens, rows), bf16),
                pltpu.VMEM((G_SLOTS, tokens, COLS), bf16),
                pltpu.VMEM((ACCS, group, piece, COLS), f32),
                pltpu.VMEM(many, bf16), pltpu.VMEM(many, bf16),
                pltpu.VMEM(one, bf16), pltpu.VMEM(one, bf16),
                pltpu.VMEM(one, bf16), pltpu.VMEM(one, bf16),
                pltpu.VMEM(one, bf16), pltpu.VMEM(one, bf16),
                dma((2, BLOCKS)), dma((G_SLOTS, BLOCKS)),
                dma((4, SLOTS)), dma((4, SLOTS)),
                dma((3, chunks)), dma((3, chunks)),
                dma((chunks,)), dma((chunks,)),
            ],
            compiler_params=pltpu.CompilerParams(collective_id=0, has_side_effects=True, vmem_limit_bytes=VMEM_LIMIT),
            cost_estimate=pl.CostEstimate(flops=flops, bytes_accessed=a.nbytes + g.nbytes, transcendentals=0),
            name="grad_sums",
        )(a.reshape(a.shape[1:]), g.reshape(g.shape[1:]))
        return sums.reshape(mats, rows, width)

    return jax.shard_map(local, mesh=mesh, in_specs=(P(("rep", "dp")),) * 2, out_specs=P("rep"), check_vma=False)


VMEM_LIMIT = 44 * 2**20
```

```python
import functools

import jax
import jax.numpy as jnp
from jax import lax
from jax.experimental import pallas as pl
from jax.experimental.pallas import tpu as pltpu
from jax.sharding import PartitionSpec as P

MESH = pl.DeviceIdType.MESH
CORES = 2
COLS = 256
SLOTS = 12
ACCS = 7
G_SLOTS = 3
AG_SLOTS = 12
EARLY = 0
LAG_A, LAG_B, LAG_C = (1, 1), (3, 3), (5, 5)
LAG_D1, LAG_E, LAG_F, LAG_G = 0, 4, 7, 9


def when(cond):
    return pl.when(cond)


def kernel(chips, mats, chunks_per, cols, a_hbm, g_hbm, out, a_buf, g_buf, acc, sib_out, sib_in, far_out, far_in,
           dir_out, dir_in, sum_out, sum_in, a_sem, first_sem, g_sem, rs_send, rs_recv, ag_send, ag_recv, pair_send, pair_recv):
    me = lax.axis_index("dp")
    x, c = me // CORES, me % CORES
    chunks = mats * chunks_per
    tokens = a_hbm.shape[1]
    rows = a_hbm.shape[2]
    piece = rows // (chips * CORES)
    cuts = [0, rows]
    split = -(-rows // 256) * 128
    partner = {"dp": x * CORES + (1 - c)}

    def chip(delta):
        return lax.rem(x + delta + chips, chips)

    def at(d):
        return {"dp": d * CORES + c}

    def ways(k):
        s = 1 - 2 * lax.rem(k, 2)
        return chip(s), chip(-s)

    far = chip(2)

    def a_copy(n):
        return pltpu.make_async_copy(a_hbm.at[n], a_buf.at[lax.rem(n, 2)], a_sem.at[lax.rem(n, 2)])

    def first_copy(i):
        part = pl.ds(cuts[i], cuts[i + 1] - cuts[i])
        return pltpu.make_async_copy(a_hbm.at[0, :, part], a_buf.at[0, :, part], first_sem.at[i])

    def g_copy(k):
        slot = lax.rem(k, G_SLOTS)
        return pltpu.make_async_copy(g_hbm.at[k // chunks_per, :, columns_of(k)], g_buf.at[slot], g_sem.at[slot])

    def columns_of(k):
        return pl.ds(pl.multiple_of(lax.rem(k, chunks_per) * cols, cols), cols)

    def remote(src, dst, send, recv, to):
        return pltpu.make_async_remote_copy(src_ref=src, dst_ref=dst, send_sem=send, recv_sem=recv, device_id=to,
                                            device_id_type=MESH)

    def rs(k, kind, src, dst, to):
        slot = lax.rem(k, SLOTS)
        return remote(src.at[slot], dst.at[slot], rs_send.at[min(kind, 1), slot], rs_recv.at[kind, slot], to)

    def swap(k):
        return rs(k, 0, sib_out, sib_in, partner)

    def hops_left(k):
        slot = lax.rem(k, SLOTS)
        three = sib_out.at[slot, pl.ds(0, 3)]
        remote(three, three, rs_send.at[1, slot], rs_recv.at[0, slot], partner).wait_send()

    def hop_far(k):
        return rs(k, 1, far_out, far_in, at(ways(k)[1]))

    def hop_direct(k):
        return rs(k, 2, dir_out, dir_in, at(ways(k)[0]))

    def hop_sum(k):
        return rs(k, 3, sum_out, sum_in, at(ways(k)[1]))

    def place(k, d):
        return out.at[k // chunks_per, d, c, :, columns_of(k)]

    def gather(k, kind, d, to):
        slot = lax.rem(k, AG_SLOTS)
        return remote(place(k, d), place(k, d), ag_send.at[slot], ag_recv.at[kind, slot], at(to))

    def pair(k):
        block = out.at[k // chunks_per, :, c, :, columns_of(k)]
        slot = lax.rem(k, AG_SLOTS)
        return remote(block, block, pair_send.at[slot], pair_recv.at[slot], partner)

    g_copy(0).start()
    for i in range(len(cuts) - 1):
        first_copy(i).start()
    barrier = pltpu.get_barrier_semaphore()
    for to in (partner, at(chip(1)), at(chip(-1))):
        pl.semaphore_signal(barrier, inc=1, device_id=to, device_id_type=MESH)

    def send_half(k):
        @when(k >= SLOTS)
        def _():
            swap(k - SLOTS).wait_send()

        for d in range(chips):
            sib_out[lax.rem(k, SLOTS), d] = terms(k, d, 1 - c).astype(jnp.bfloat16)
        swap(k).start()

    def terms(k, d, core):
        return acc[lax.rem(k, ACCS), pl.ds(pl.multiple_of((d * CORES + core) * piece, piece), piece)]

    def multiply(k, tokens_of, rows_of):
        return lax.dot_general(a_buf[lax.rem(k // chunks_per, 2), tokens_of, rows_of], g_buf[lax.rem(k, G_SLOTS), tokens_of],
                               (((0,), (0,)), ((), ())), preferred_element_type=jnp.float32)

    def start_loads(k):
        @when(k < chunks)
        def _():
            g_copy(k).start()

    def ready(k):
        n, first = k // chunks_per, lax.rem(k, chunks_per) == 0

        @when(first & (n + 1 < mats))
        def _():
            a_copy(n + 1).start()

        @when(first)
        def _():
            a_copy(n).wait()

        g_copy(k).wait()

    def part_matmul(k, lo, hi):
        acc[lax.rem(k, ACCS), pl.ds(lo, hi - lo)] = multiply(k, pl.ds(0, tokens), pl.ds(lo, hi - lo))

    def mine(k, d):
        return terms(k, d, c) + sib_in[lax.rem(k, SLOTS), d].astype(jnp.float32)

    def stage_a(k):
        slot = lax.rem(k, SLOTS)
        swap(k).wait_recv()

        @when(k >= SLOTS)
        def _():
            hops_left(k - SLOTS)

        far_out[slot] = mine(k, far).astype(jnp.bfloat16)
        hop_far(k).start()
        dir_out[slot] = mine(k, ways(k)[0]).astype(jnp.bfloat16)
        hop_direct(k).start()

    def stage_b(k):
        slot = lax.rem(k, SLOTS)
        hop_far(k).wait_recv()
        sum_out[slot] = (mine(k, ways(k)[1]) + far_in[slot].astype(jnp.float32)).astype(jnp.bfloat16)
        hop_sum(k).start()

    def stage_c(k):
        slot = lax.rem(k, SLOTS)
        hop_direct(k).wait_recv()
        hop_sum(k).wait_recv()
        total = mine(k, x) + dir_in[slot].astype(jnp.float32) + sum_in[slot].astype(jnp.float32)
        place(k, x)[...] = total.astype(jnp.bfloat16)

    def stage_d(k):
        gather(k, 0, x, ways(k)[0]).start()

    def stage_d1(k):
        gather(k, 1, x, ways(k)[1]).start()

    def stage_e(k):
        forth, back = ways(k)
        gather(k, 0, back, forth).wait_recv()
        gather(k, 2, back, forth).start()
        gather(k, 1, forth, back).wait_recv()

    def stage_f(k):
        forth, back = ways(k)
        gather(k, 2, far, forth).wait_recv()
        pair(k).start()

    def stage_g(k):
        block = out.at[k // chunks_per, pl.ds(0, 3), c, :, columns_of(k)]
        slot = lax.rem(k, AG_SLOTS)
        remote(block, block, ag_send.at[slot], ag_recv.at[0, slot], partner).wait_send()
        pair(k).wait_recv()
        pair(k).wait_send()

    def spread(t):
        return (t // 1) * 1 + lax.rem(t, 1), lax.rem(t, 1) < 1

    def stages(t):
        for stage, (early, late) in ((stage_b, LAG_B), (stage_c, LAG_C)):
            soon, k = t - early < EARLY, t - late
            k = jnp.where(soon, t - early, k)

            @when((k >= 0) & (k < chunks) & (soon | (k >= EARLY)))
            def _():
                stage(k)

        for stage, lag in ((stage_d, 0), (stage_d1, LAG_D1), (stage_e, LAG_E), (stage_f, LAG_F), (stage_g, LAG_G)):
            u = t - lag - LAG_C[0]
            k, there = spread(jnp.maximum(u, 0))

            @when((u >= 0) & there & (k < chunks))
            def _():
                stage(k)

    def tick(t, _):
        busy = t < chunks

        @when(busy)
        def _():
            pass

        stages(t)

        @when(busy)
        def _():
            start_loads(t + 2)
            ready(t)
            part_matmul(t, 0, split)

        @when((t >= 1) & (t <= chunks))
        def _():
            stage_a(t - 1)

        @when(busy)
        def _():
            part_matmul(t, split, rows)
            send_half(t)

        @when(t == chunks + LAG_C[1] + 1)
        def _():
            def drain(i, _):
                k = chunks - SLOTS + i
                swap(k).wait_send()
                hops_left(k)
                return 0

            lax.fori_loop(0, SLOTS, drain, 0)

        return 0

    start_loads(1)
    g_copy(0).wait()
    for i in range(len(cuts) - 1):
        first_copy(i).wait()
        part_matmul(0, cuts[i], cuts[i + 1])
        if i == 0:
            start_loads(2)
    a_copy(1).start()
    pl.semaphore_wait(barrier, 3)
    send_half(0)
    last = ((chunks - 1) // 1) * 1 + (chunks - 1) % 1
    lax.fori_loop(1, LAG_C[0] + last + LAG_G + 1, tick, 0)


def solution(mesh):
    group = mesh.shape["dp"]
    chips = group // CORES

    def local(a, g):
        _, mats, tokens, rows = a.shape
        width = g.shape[-1]
        piece = rows // group
        chunks_per = width // COLS
        chunks = mats * chunks_per
        shape = (mats, chips, CORES, piece, width)
        bf16, f32 = jnp.bfloat16, jnp.float32
        many, one = (SLOTS, chips, piece, COLS), (SLOTS, piece, COLS)
        dma = pltpu.SemaphoreType.DMA
        flops = 2 * mats * tokens * rows * width
        sums = pl.pallas_call(
            functools.partial(kernel, chips, mats, chunks_per, COLS),
            out_shape=pltpu.VMEM(shape, bf16),
            in_specs=[pl.BlockSpec(memory_space=pl.ANY)] * 2,
            out_specs=pl.BlockSpec(memory_space=pltpu.VMEM),
            scratch_shapes=[
                pltpu.VMEM((2, tokens, rows), bf16),
                pltpu.VMEM((G_SLOTS, tokens, COLS), bf16),
                pltpu.VMEM((ACCS, rows, COLS), f32),
                pltpu.VMEM(many, bf16), pltpu.VMEM(many, bf16),
                pltpu.VMEM(one, bf16), pltpu.VMEM(one, bf16),
                pltpu.VMEM(one, bf16), pltpu.VMEM(one, bf16),
                pltpu.VMEM(one, bf16), pltpu.VMEM(one, bf16),
                dma((2,)), dma((1,)), dma((G_SLOTS,)),
                dma((2, SLOTS)), dma((4, SLOTS)),
                dma((AG_SLOTS,)), dma((3, AG_SLOTS)),
                dma((AG_SLOTS,)), dma((AG_SLOTS,)),
            ],
            compiler_params=pltpu.CompilerParams(collective_id=0, has_side_effects=True, vmem_limit_bytes=VMEM_LIMIT),
            cost_estimate=pl.CostEstimate(flops=flops, bytes_accessed=a.nbytes + g.nbytes, transcendentals=0),
            name="grad_sums",
        )(a.reshape(a.shape[1:]), g.reshape(g.shape[1:]))
        return sums.reshape(mats, rows, width)

    return jax.shard_map(local, mesh=mesh, in_specs=(P(("rep", "dp")),) * 2, out_specs=P("rep"), check_vma=False)


VMEM_LIMIT = 44 * 2**20
```

```python
import functools

import jax
import jax.numpy as jnp
from jax import lax
from jax.experimental import pallas as pl
from jax.experimental.pallas import tpu as pltpu
from jax.sharding import PartitionSpec as P

MESH = pl.DeviceIdType.MESH
CORES = 2
COLS = 256
BLOCKS = 4
SLOTS = 12
ACCS = 7
G_SLOTS = 3
AG_SLOTS = 12
LAG_A, LAG_B, LAG_C = 1, 3, 5
LAG_E, LAG_F, LAG_G = 4, 8, 10


def kernel(chips, mats, chunks_per, cols, a_hbm, g_hbm, out, a_buf, g_buf, acc, sib_out, sib_in, far_out, far_in,
           dir_out, dir_in, sum_out, sum_in, a_sem, first_sem, g_sem, rs_send, rs_recv, ag_send, ag_recv, pair_send, pair_recv):
    me = lax.axis_index("dp")
    x, c = me // CORES, me % CORES
    chunks = mats * chunks_per
    tokens = a_hbm.shape[1]
    rows = a_hbm.shape[2]
    piece = rows // (chips * CORES)
    step = tokens // BLOCKS
    split = -(-rows // 256) * 128
    partner = {"dp": x * CORES + (1 - c)}

    def chip(delta):
        return lax.rem(x + delta + chips, chips)

    def at(d):
        return {"dp": d * CORES + c}

    def ways(k):
        s = 1 - 2 * lax.rem(k, 2)
        return chip(s), chip(-s)

    far = chip(chips // 2)

    def a_copy(n):
        return pltpu.make_async_copy(a_hbm.at[n], a_buf.at[lax.rem(n, 2)], a_sem.at[lax.rem(n, 2)])

    def first_copies(b):
        part = pl.ds(pl.multiple_of(b * step, step), step)
        return (pltpu.make_async_copy(a_hbm.at[0, part], a_buf.at[0, part], first_sem.at[0, b]),
                pltpu.make_async_copy(g_hbm.at[0, part, pl.ds(0, cols)], g_buf.at[0, part], first_sem.at[1, b]))

    def g_copy(k):
        slot = lax.rem(k, G_SLOTS)
        return pltpu.make_async_copy(g_hbm.at[k // chunks_per, :, columns_of(k)], g_buf.at[slot], g_sem.at[slot])

    def columns_of(k):
        return pl.ds(pl.multiple_of(lax.rem(k, chunks_per) * cols, cols), cols)

    def remote(src, dst, send, recv, to):
        return pltpu.make_async_remote_copy(src_ref=src, dst_ref=dst, send_sem=send, recv_sem=recv, device_id=to,
                                            device_id_type=MESH)

    def rs(k, kind, src, dst, to):
        slot = lax.rem(k, SLOTS)
        return remote(src.at[slot], dst.at[slot], rs_send.at[min(kind, 1), slot], rs_recv.at[kind, slot], to)

    def swap(k):
        return rs(k, 0, sib_out, sib_in, partner)

    def hops_left(k):
        slot = lax.rem(k, SLOTS)
        three = sib_out.at[slot, pl.ds(0, 3)]
        remote(three, three, rs_send.at[1, slot], rs_recv.at[0, slot], partner).wait_send()

    def hop_far(k):
        return rs(k, 1, far_out, far_in, at(ways(k)[1]))

    def hop_direct(k):
        return rs(k, 2, dir_out, dir_in, at(ways(k)[0]))

    def hop_sum(k):
        return rs(k, 3, sum_out, sum_in, at(ways(k)[1]))

    def place(k, d):
        return out.at[k // chunks_per, d, c, :, columns_of(k)]

    def gather(k, kind, d, to):
        slot = lax.rem(k, AG_SLOTS)
        return remote(place(k, d), place(k, d), ag_send.at[slot], ag_recv.at[kind, slot], at(to))

    def pair(k):
        block = out.at[k // chunks_per, :, c, :, columns_of(k)]
        slot = lax.rem(k, AG_SLOTS)
        return remote(block, block, pair_send.at[slot], pair_recv.at[slot], partner)

    for b in range(BLOCKS):
        for copy in first_copies(b):
            copy.start()
    barrier = pltpu.get_barrier_semaphore()
    for to in (partner, at(chip(1)), at(chip(-1))):
        pl.semaphore_signal(barrier, inc=1, device_id=to, device_id_type=MESH)

    def send_half(k):
        @pl.when(k >= SLOTS)
        def _():
            swap(k - SLOTS).wait_send()

        for d in range(chips):
            sib_out[lax.rem(k, SLOTS), d] = terms(k, d, 1 - c).astype(jnp.bfloat16)
        swap(k).start()

    def terms(k, d, core):
        return acc[lax.rem(k, ACCS), pl.ds(pl.multiple_of((d * CORES + core) * piece, piece), piece)]

    def multiply(k, tokens_of, rows_of):
        return lax.dot_general(a_buf[lax.rem(k // chunks_per, 2), tokens_of, rows_of], g_buf[lax.rem(k, G_SLOTS), tokens_of],
                               (((0,), (0,)), ((), ())), preferred_element_type=jnp.float32)

    def start_loads(k):
        @pl.when(k < chunks)
        def _():
            g_copy(k).start()

    def ready(k):
        n, first = k // chunks_per, lax.rem(k, chunks_per) == 0

        @pl.when(first & (n + 1 < mats))
        def _():
            a_copy(n + 1).start()

        @pl.when(first)
        def _():
            a_copy(n).wait()

        g_copy(k).wait()

    def part_matmul(k, lo, hi):
        acc[lax.rem(k, ACCS), pl.ds(lo, hi - lo)] = multiply(k, pl.ds(0, tokens), pl.ds(lo, hi - lo))

    def mine(k, d):
        return terms(k, d, c) + sib_in[lax.rem(k, SLOTS), d].astype(jnp.float32)

    def stage_a(k):
        slot = lax.rem(k, SLOTS)
        swap(k).wait_recv()

        @pl.when(k >= SLOTS)
        def _():
            hops_left(k - SLOTS)

        far_out[slot] = mine(k, far).astype(jnp.bfloat16)
        hop_far(k).start()
        dir_out[slot] = mine(k, ways(k)[0]).astype(jnp.bfloat16)
        hop_direct(k).start()

    def stage_b(k):
        slot = lax.rem(k, SLOTS)
        hop_far(k).wait_recv()
        sum_out[slot] = (mine(k, ways(k)[1]) + far_in[slot].astype(jnp.float32)).astype(jnp.bfloat16)
        hop_sum(k).start()

    def stage_c(k):
        slot = lax.rem(k, SLOTS)
        hop_direct(k).wait_recv()
        hop_sum(k).wait_recv()
        total = mine(k, x) + dir_in[slot].astype(jnp.float32) + sum_in[slot].astype(jnp.float32)
        place(k, x)[...] = total.astype(jnp.bfloat16)

    def stage_d(k):
        gather(k, 0, x, ways(k)[0]).start()
        gather(k, 1, x, ways(k)[1]).start()

    def stage_e(k):
        forth, back = ways(k)
        gather(k, 0, back, forth).wait_recv()
        gather(k, 2, back, forth).start()
        gather(k, 1, forth, back).wait_recv()

    def stage_f(k):
        forth, back = ways(k)
        gather(k, 2, far, forth).wait_recv()
        pair(k).start()

    def stage_g(k):
        block = out.at[k // chunks_per, pl.ds(0, 3), c, :, columns_of(k)]
        slot = lax.rem(k, AG_SLOTS)
        remote(block, block, ag_send.at[slot], ag_recv.at[0, slot], partner).wait_send()
        pair(k).wait_recv()
        pair(k).wait_send()

    def stages(t):
        lags = ((stage_b, LAG_B), (stage_c, LAG_C), (stage_d, LAG_C), (stage_e, LAG_C + LAG_E), (stage_f, LAG_C + LAG_F),
                (stage_g, LAG_C + LAG_G))
        for stage, lag in lags:
            k = t - lag

            @pl.when((k >= 0) & (k < chunks))
            def _():
                stage(k)

    def tick(t, _):
        busy = t < chunks

        stages(t)

        @pl.when(busy)
        def _():
            start_loads(t + 2)
            ready(t)
            part_matmul(t, 0, split)

        @pl.when(t - LAG_A < chunks)
        def _():
            stage_a(t - LAG_A)

        @pl.when(busy)
        def _():
            part_matmul(t, split, rows)
            send_half(t)

        @pl.when(t == chunks + LAG_C + 1)
        def _():
            def drain(i, _):
                k = chunks - SLOTS + i
                swap(k).wait_send()
                hops_left(k)
                return 0

            lax.fori_loop(0, SLOTS, drain, 0)

        return 0

    acc[0] = jnp.zeros(acc.shape[1:], jnp.float32)

    def first_part(b, _):
        for copy in first_copies(b):
            copy.wait()

        @pl.when(b == BLOCKS // 2)
        def _():
            start_loads(1)

        acc[0] += multiply(0, pl.ds(pl.multiple_of(b * step, step), step), pl.ds(0, rows))
        return 0

    lax.fori_loop(0, BLOCKS, first_part, 0)
    start_loads(2)
    a_copy(1).start()
    pl.semaphore_wait(barrier, 3)
    send_half(0)
    lax.fori_loop(1, chunks + LAG_C + LAG_G, tick, 0)


def settle(parts, sums, out, sem):
    def copy(i):
        at = i // sums.shape[1], i % sums.shape[1]
        return pltpu.make_async_copy(sums.at[at], out.at[at], sem.at[i])

    for i in range(parts):
        copy(i).start()
    for i in range(parts):
        copy(i).wait()


def solution(mesh):
    group = mesh.shape["dp"]
    chips = group // CORES

    def local(a, g):
        _, mats, tokens, rows = a.shape
        width = g.shape[-1]
        piece = rows // group
        chunks_per = width // COLS
        chunks = mats * chunks_per
        shape = (mats, chips, CORES, piece, width)
        bf16, f32 = jnp.bfloat16, jnp.float32
        many, one = (SLOTS, chips, piece, COLS), (SLOTS, piece, COLS)
        dma = pltpu.SemaphoreType.DMA
        flops = 2 * mats * tokens * rows * width
        sums = pl.pallas_call(
            functools.partial(kernel, chips, mats, chunks_per, COLS),
            out_shape=pltpu.VMEM(shape, bf16),
            in_specs=[pl.BlockSpec(memory_space=pl.ANY)] * 2,
            out_specs=pl.BlockSpec(memory_space=pltpu.VMEM),
            scratch_shapes=[
                pltpu.VMEM((2, tokens, rows), bf16),
                pltpu.VMEM((G_SLOTS, tokens, COLS), bf16),
                pltpu.VMEM((ACCS, rows, COLS), f32),
                pltpu.VMEM(many, bf16), pltpu.VMEM(many, bf16),
                pltpu.VMEM(one, bf16), pltpu.VMEM(one, bf16),
                pltpu.VMEM(one, bf16), pltpu.VMEM(one, bf16),
                pltpu.VMEM(one, bf16), pltpu.VMEM(one, bf16),
                dma((2,)), dma((2, BLOCKS)), dma((G_SLOTS,)),
                dma((2, SLOTS)), dma((4, SLOTS)),
                dma((AG_SLOTS,)), dma((3, AG_SLOTS)),
                dma((AG_SLOTS,)), dma((AG_SLOTS,)),
            ],
            compiler_params=pltpu.CompilerParams(collective_id=0, has_side_effects=True, vmem_limit_bytes=VMEM_LIMIT),
            cost_estimate=pl.CostEstimate(flops=flops, bytes_accessed=a.nbytes + g.nbytes, transcendentals=0),
            name="grad_sums",
        )(a.reshape(a.shape[1:]), g.reshape(g.shape[1:]))
        whole = pl.pallas_call(
            functools.partial(settle, mats * chips),
            out_shape=jax.ShapeDtypeStruct(shape, bf16),
            in_specs=[pl.BlockSpec(memory_space=pltpu.VMEM)],
            out_specs=pl.BlockSpec(memory_space=pl.ANY),
            scratch_shapes=[dma((mats * chips,))],
            compiler_params=pltpu.CompilerParams(vmem_limit_bytes=2**20),
            name="settle",
        )(pltpu.with_memory_space_constraint(sums, pltpu.VMEM))
        return whole.reshape(mats, rows, width)

    return jax.shard_map(local, mesh=mesh, in_specs=(P(("rep", "dp")),) * 2, out_specs=P("rep"), check_vma=False)


VMEM_LIMIT = 44 * 2**20
```
